32 devices in a mesh: expert: 8 (over z, x), tensor: 4 (over y, core).
Axes of the slice: x: 2, y: 2, z: 4, core: 2. Of those that a mesh axis runs over, the one named last changes fastest.
Arguments:
- tokens: bfloat16 [1024, 3584], P('expert', 'tensor'), may hold values from -6 to 6
- expert_ids: int32 [1024, 4], P('expert'), may hold values from 0 to 7, all different within a row; in each aligned block of 128 rows (0 to 127, 128 to 255, ...) at most 96 rows name the same one
- gate_values: bfloat16 [1024, 4], P('expert'), may hold values from 0.049804688 to 0.3984375
- w_gate: bfloat16 [8, 3584, 1024], P('expert', None, 'tensor'), may hold values from -0.09375 to 0.09375
- w_up: bfloat16 [8, 3584, 1024], P('expert', None, 'tensor'), may hold values from -0.09375 to 0.09375
- w_down: bfloat16 [8, 1024, 3584], P('expert', 'tensor'), may hold values from -0.1875 to 0.1875
- shared_gate: bfloat16 [3584, 1024], P(None, 'tensor'), may hold values from -0.09375 to 0.09375
- shared_up: bfloat16 [3584, 1024], P(None, 'tensor'), may hold values from -0.09375 to 0.09375
- shared_down: bfloat16 [1024, 3584], P('tensor'), may hold values from -0.1875 to 0.1875
Outputs:
- moe_output: bfloat16 [1024, 3584], P('expert', 'tensor')
The draws below stay inside these ranges and needn't reach their ends.
Inputs may be any that keep to these rules, and one draw needn't show every extreme that they name: `expert_ids`: each token names 4 different experts. Among the 128 tokens of one index of the expert axis (aligned blocks of 128 rows) no expert is named by more than 96 tokens, a bound that some block reaches.
All inputs are finite; a program needn't handle non-finite values.
Results may differ from the reference program's by a relative error of at most 0.013.
Values may be sent and summed in bfloat16 or wider, within the bound.
A program may use at most 64 MiB of HBM per device.

```python
import math
import jax
import jax.numpy as jnp
import numpy as np
from jax import lax

D = 3584
FF = 1024
SFF = 1024
TOPK = 4
TOK_DEV = 128
EXPERTS = 8
CAP = 96
TOKENS = 1024
N_TENSOR = 4


def block_scale(key, shape, pieces, smallest, largest):
    level = 1.0
    for axis_at, shards_of in pieces:
        steps = jax.random.uniform(jax.random.fold_in(jax.random.fold_in(key, 6), axis_at), (shards_of,), jnp.float32, smallest / len(pieces), largest / len(pieces))
        level = level * jnp.repeat(jnp.exp(steps), shape[axis_at] // shards_of).reshape((-1,) + (1,) * (len(shape) - 1 - axis_at))
    return level


def assign_block(rng, own, number, rows, number_of, top, limit, lean):
    order = jax.random.permutation(rng, number_of)
    crowded, usual = load_shares(number_of, rows * top, limit, lean, True), load_shares(number_of, rows * top, limit, lean, False)
    places = jnp.arange(number_of)

    def named(lengths, turn):
        used = int((lengths > 0).sum())
        fixed = max(1, used // 4)
        passed = fixed + (places - fixed + turn * (used - fixed)) % max(1, number_of - fixed)
        return jnp.zeros((number_of,), jnp.int32).at[order[jnp.where(places < fixed, places, passed)]].set(jnp.asarray(lengths, jnp.int32))

    lengths = jnp.where(number % 4 == 0, named(crowded, number // 4), named(usual, number - number // 4 - 1))
    mixed = jax.random.permutation(jax.random.fold_in(own, 3), number_of)
    source_of, receiver = mixed[0:number_of // 2 * 2:2], mixed[1:number_of // 2 * 2:2]
    slack = jnp.minimum(lengths[source_of] - 1, limit - lengths[receiver]) // 2
    slack = jnp.where((source_of == order[0]) | (receiver == order[0]) | (lengths[receiver] == 0), 0, jnp.maximum(slack, 0))
    passed = jax.random.randint(jax.random.fold_in(own, 4), (number_of // 2,), 0, 1 << 20) % (slack + 1)
    lengths = lengths.at[source_of].add(-passed).at[receiver].add(passed)
    items = jnp.searchsorted(jnp.cumsum(lengths), jnp.arange(rows * top), side="right").astype(jnp.int32)
    listing = items.reshape(top, rows).T
    listing = listing[jax.random.permutation(jax.random.fold_in(own, 1), rows)]
    turn = jax.random.randint(jax.random.fold_in(own, 2), (rows, 1), 0, top)
    return jnp.take_along_axis(listing, (jnp.arange(top)[None, :] + turn) % top, axis=1)


def load_shares(amount, total, limit, skew, full):
    portions = [(1 << 20) // math.isqrt(grade ** skew) + 1 for grade in range(1, amount + 1)]
    largest = limit if full else min(limit, max(-(-total // amount), total * portions[0] // sum(portions)))
    least = 1 if total - largest >= amount - 1 else 0
    counts, rest = [largest] + [least] * (amount - 1), total - largest - least * (amount - 1)
    while rest > 0:
        movable = [i for i in range(1, amount) if counts[i] < largest] or [i for i in range(1, amount) if counts[i] < limit]
        mass, left = sum([portions[i] for i in movable]), rest
        for i in movable:
            more = min(limit - counts[i], max(1, left * portions[i] // mass), rest)
            counts[i] = counts[i] + more
            rest = rest - more
    return np.array(counts)


def gaussian(own_key, extent, width, limit, cuts=(), kind=jnp.bfloat16):
    gain = block_scale(own_key, extent, cuts, -0.22, 0.18) if cuts else 1.0
    entries = jax.random.normal(own_key, extent, jnp.float32) * width * gain
    return jnp.minimum(jnp.maximum(entries, -limit), limit).astype(kind)


def setup_inputs(seed: int = 0) -> dict:
    key_list = jax.random.split(jax.random.key(seed), 10)
    tokens = gaussian(key_list[0], (TOKENS, D), 1.0, 6.0, ((0, 8), (1, 4)))
    expert_ids_keys = jax.random.split(jax.random.fold_in(key_list[1], 1), TOKENS // TOK_DEV)
    expert_ids_turns = jax.random.permutation(jax.random.fold_in(key_list[1], 3), TOKENS // TOK_DEV)
    expert_ids = jax.vmap(lambda own, number: assign_block(jax.random.fold_in(key_list[1], 2), own, number, TOK_DEV, EXPERTS, TOPK, CAP, 2))(expert_ids_keys, expert_ids_turns).reshape((TOKENS, TOPK))
    gate_values = jnp.clip(0.049804688 + 0.3486328 * jax.random.uniform(key_list[2], (TOKENS, TOPK), jnp.float32) ** block_scale(key_list[2], (TOKENS, TOPK), ((0, 8),), -0.2, 0.2), 0.049804688, 0.3984375).astype(jnp.bfloat16)
    w_gate = gaussian(key_list[3], (EXPERTS, D, FF), D ** -0.5, 0.09375, ((0, 8), (2, 4)))
    w_up = gaussian(key_list[4], (EXPERTS, D, FF), D ** -0.5, 0.09375, ((0, 8), (2, 4)))
    w_down = gaussian(key_list[5], (EXPERTS, FF, D), FF ** -0.5, 0.1875, ((0, 8), (1, 4)))
    shared_gate = gaussian(key_list[6], (D, SFF), D ** -0.5, 0.09375, ((1, 4),))
    shared_up = gaussian(key_list[7], (D, SFF), D ** -0.5, 0.09375, ((1, 4),))
    shared_down = gaussian(key_list[8], (SFF, D), SFF ** -0.5, 0.1875, ((0, 4),))
    return dict(tokens=tokens, expert_ids=expert_ids, gate_values=gate_values, w_gate=w_gate, w_up=w_up, w_down=w_down, shared_gate=shared_gate, shared_up=shared_up, shared_down=shared_down)


def reference(tokens, expert_ids, gate_values, w_gate, w_up, w_down, shared_gate, shared_up, shared_down):
    block_count = TOKENS // TOK_DEV
    slot_rows = block_count * CAP
    quarter = FF // N_TENSOR
    numbers = jnp.arange(EXPERTS, dtype=jnp.int32)
    grouped = expert_ids.reshape(block_count, TOK_DEV, TOPK)
    onehot = (grouped[..., None] == numbers).astype(jnp.int32)
    per_token = jnp.sum(onehot, axis=2)
    earlier = jnp.cumsum(per_token, axis=1) - per_token
    slot_index = jnp.sum(onehot * earlier[:, :, None, :], axis=3)
    position = (jnp.arange(block_count, dtype=jnp.int32)[:, None, None] * CAP + slot_index).reshape(TOKENS, TOPK)
    token_index = jnp.arange(TOKENS, dtype=jnp.int32)
    padded = jnp.concatenate([tokens, jnp.zeros((1, D), tokens.dtype)], axis=0)
    gate_float = gate_values.astype(jnp.float32)

    def one_expert(combined, inputs):
        gate_matrix, up_matrix, down_matrix, number = inputs
        chosen = expert_ids == number
        location = jnp.sum(jnp.where(chosen, position, 0), axis=1).astype(jnp.int32)
        weight = jnp.sum(jnp.where(chosen, gate_float, 0.0), axis=1)
        used = jnp.any(chosen, axis=1)
        owners = jnp.full((slot_rows,), TOKENS, jnp.int32)
        owners = owners.at[jnp.where(used, location, slot_rows).astype(jnp.int32)].set(token_index, mode="drop")
        rows = padded[owners].astype(jnp.float32)
        gate_sums = jnp.dot(rows, gate_matrix.astype(jnp.float32), precision=lax.Precision.HIGHEST)
        up_sums = jnp.dot(rows, up_matrix.astype(jnp.float32), precision=lax.Precision.HIGHEST)
        hidden = (jax.nn.silu(gate_sums) * up_sums).astype(jnp.bfloat16)
        blocks = jnp.einsum("rqf,qfd->rqd", hidden.reshape(slot_rows, N_TENSOR, quarter).astype(jnp.float32),
                            down_matrix.reshape(N_TENSOR, quarter, D).astype(jnp.float32),
                            precision=lax.Precision.HIGHEST)
        rounded = lax.optimization_barrier(blocks.astype(jnp.bfloat16))
        expert_out = jnp.sum(rounded.astype(jnp.float32), axis=1)
        picked = expert_out[jnp.minimum(location, slot_rows - 1)]
        return combined + weight[:, None] * picked, None

    start = jnp.zeros((TOKENS, D), jnp.float32)
    routed, unused = lax.scan(one_expert, start, (w_gate, w_up, w_down, numbers))
    token_float = tokens.astype(jnp.float32)
    shared_hidden = (jax.nn.silu(jnp.dot(token_float, shared_gate.astype(jnp.float32), precision=lax.Precision.HIGHEST))
                     * jnp.dot(token_float, shared_up.astype(jnp.float32), precision=lax.Precision.HIGHEST)).astype(jnp.bfloat16)
    shared_out = jnp.dot(shared_hidden, shared_down, preferred_element_type=jnp.float32)
    return (routed + shared_out).astype(jnp.bfloat16)
```

```python
import functools

import jax
import jax.numpy as jnp
from jax import lax
from jax.experimental import pallas as pl
from jax.experimental.pallas import tpu as pltpu
from jax.sharding import PartitionSpec as P

MESH = pl.DeviceIdType.MESH
F32 = jnp.float32
BF16 = jnp.bfloat16


def capacity_of(tok_dev, top_count, experts_all):
    return min(tok_dev, 3 * tok_dev * top_count // (2 * experts_all))


def dispatch_form(
    tokens, expert_ids, gate_values, w_gate, w_up, w_down, shared_gate, shared_up, shared_down
):
    tok_dev, narrow = tokens.shape
    top_count = expert_ids.shape[1]
    per_lane, features, quarter = w_gate.shape
    lane_count = lax.axis_size("expert")
    experts_all = lane_count * per_lane
    capacity = min(tok_dev, 3 * tok_dev * top_count // (2 * experts_all))
    total_rows = experts_all * capacity
    numbers = jnp.arange(experts_all, dtype=jnp.int32)
    onehot = (expert_ids[:, :, None] == numbers).astype(jnp.int32)
    per_token = jnp.sum(onehot, axis=1)
    earlier = jnp.cumsum(per_token, axis=0) - per_token
    slot_index = jnp.sum(onehot * earlier[:, None, :], axis=2)
    target = expert_ids * capacity + slot_index
    token_index = jnp.repeat(jnp.arange(tok_dev, dtype=jnp.int32), top_count)
    owners = jnp.full((total_rows,), tok_dev, jnp.int32).at[target.reshape(-1)].set(token_index)
    features_all = lax.all_gather(tokens, "tensor", axis=1, tiled=True)
    shared_gate_sums = jnp.dot(features_all, shared_gate, preferred_element_type=jnp.float32)
    shared_up_sums = jnp.dot(features_all, shared_up, preferred_element_type=jnp.float32)
    shared_hidden = (jax.nn.silu(shared_gate_sums) * shared_up_sums).astype(jnp.bfloat16)
    shared_partial = jnp.dot(shared_hidden, shared_down, preferred_element_type=jnp.float32)
    padded = jnp.concatenate([tokens, jnp.zeros((1, narrow), jnp.bfloat16)], axis=0)
    outgoing = padded[owners].reshape(lane_count, per_lane * capacity, narrow)
    arrived = lax.all_to_all(outgoing, "expert", split_axis=0, concat_axis=0, tiled=True)
    arrived = arrived.reshape(lane_count, per_lane, capacity, narrow)
    block_rows = lax.all_gather(arrived, "tensor", axis=3, tiled=True)
    gate_more = jnp.einsum("sjcd,jdf->sjcf", block_rows, w_gate, preferred_element_type=jnp.float32)
    up_more = jnp.einsum("sjcd,jdf->sjcf", block_rows, w_up, preferred_element_type=jnp.float32)
    hidden = (jax.nn.silu(gate_more) * up_more).astype(jnp.bfloat16)
    partial_value = jnp.einsum("sjcf,jfd->sjcd", hidden, w_down, preferred_element_type=jnp.float32)
    summed = lax.psum_scatter(
        partial_value.astype(jnp.bfloat16), "tensor", scatter_dimension=3, tiled=True
    ).astype(jnp.float32)
    returned = lax.all_to_all(
        summed.reshape(lane_count, per_lane * capacity, narrow).astype(jnp.bfloat16),
        "expert",
        split_axis=0,
        concat_axis=0,
        tiled=True,
    ).astype(jnp.float32)
    picked = returned.reshape(total_rows, narrow)[target]
    routed = jnp.sum(gate_values.astype(jnp.float32)[:, :, None] * picked, axis=1)
    shared_total = lax.psum_scatter(
        shared_partial.astype(jnp.bfloat16), "tensor", scatter_dimension=1, tiled=True
    ).astype(jnp.float32)
    return (routed + shared_total).astype(jnp.bfloat16)


def layer_kernel(
    lanes, tok_hbm, wt_hbm, wg_hbm, wu_hbm, wd_hbm, sg_hbm, su_hbm, sd_hbm, out_ref,
    xbuf, wtb, wg, wu, wd, sg, su, sd, shared_hidden, part, got_core, got_h0, got_h1,
    got_x, got_y, got_z, load_sem, send_sem, recv_sem,
):
    planes = lanes // 2
    rows, narrow = out_ref.shape
    half, both = rows // 2, 2 * rows
    quarter = wg.shape[1]
    lane, tens = lax.axis_index("expert"), lax.axis_index("tensor")
    z, x = lane // 2, lax.rem(lane, 2)
    y, c = tens // 2, lax.rem(tens, 2)
    ox, oy, oc = 1 - x, 1 - y, 1 - c
    up = lax.rem(z + 1, planes)
    down = lax.rem(z + planes - 1, planes)
    at_core = (lane, y * 2 + oc)
    at_x = (z * 2 + ox, tens)
    at_y = (lane, oy * 2 + c)
    at_up = (up * 2 + x, tens)
    at_down = (down * 2 + x, tens)
    tens_y = oy * 2 + c
    number, copies = {}, {}

    def send(key, src, dst, device):
        k = number.setdefault(key, len(number))
        copies[key] = pltpu.make_async_remote_copy(
            src_ref=src, dst_ref=dst, send_sem=send_sem.at[k], recv_sem=recv_sem.at[k],
            device_id=device, device_id_type=MESH)
        copies[key].start()

    def arrived(key):
        copies[key].wait_recv()

    def span(start, size):
        return pl.ds(pl.multiple_of(start, size), size)

    def piece(t, plane, ix):
        return xbuf.at[t, span((plane * 2 + ix) * rows, rows), :]

    def half_piece(t, plane, ix, h):
        return xbuf.at[t, span((plane * 2 + ix) * rows + h * half, half), :]

    loads = []
    for src, dst in (
        (tok_hbm, piece(tens, z, x)), (wt_hbm, wtb.at[lane]), (wg_hbm, wg), (wu_hbm, wu),
        (sg_hbm, sg), (su_hbm, su), (wd_hbm, wd), (sd_hbm, sd),
    ):
        copy = pltpu.make_async_copy(src, dst, load_sem.at[len(loads)])
        copy.start()
        loads.append(copy)

    barrier = pltpu.get_barrier_semaphore()
    for device in (at_core, at_x, at_y, at_up, at_down):
        pl.semaphore_signal(barrier, inc=1, device_id=device, device_id_type=MESH)
    pl.semaphore_wait(barrier, 5)

    def plane_at(s):
        return lax.rem(z - s + planes, planes)

    def issue(s):
        p = plane_at(s)
        if s == 0:
            loads[0].wait()
            loads[1].wait()
        else:
            arrived(("z", s - 1))
            arrived(("wz", s - 1))
        mine, weight = piece(tens, p, x), wtb.at[p * 2 + x]
        if s < planes - 1:
            send(("z", s), mine, mine, at_up)
            send(("wz", s), weight, weight, at_up)
        send(("x", s), mine, mine, at_x)
        send(("y", s), mine, mine, at_y)
        send(("wx", s), weight, weight, at_x)
        send(("c", s), mine, mine, at_core)

    def forward(s):
        p = plane_at(s)
        arrived(("x", s))
        first = half_piece(tens, p, ox, 0)
        send(("d0", s), first, first, at_y)
        other = piece(tens, p, ox)
        send(("cx", s), other, other, at_core)
        arrived(("y", s))
        second = half_piece(tens_y, p, x, 1)
        send(("d1", s), second, second, at_x)
        other = piece(tens_y, p, x)
        send(("cy", s), other, other, at_core)

    def finish(s):
        p = plane_at(s)
        arrived(("d0", s))
        arrived(("d1", s))
        far = piece(tens_y, p, ox)
        send(("cd", s), far, far, at_core)
        arrived(("wx", s))
        for key in ("c", "cx", "cy", "cd"):
            arrived((key, s))

    tensors = xbuf.shape[0]

    def hidden_of(start, count, gate_matrix, up_matrix):
        gate_sums = up_sums = None
        for t in range(tensors):
            block = xbuf[t, span(start, count), :]
            g = jnp.dot(block, gate_matrix[t * narrow:(t + 1) * narrow, :], preferred_element_type=F32)
            u = jnp.dot(block, up_matrix[t * narrow:(t + 1) * narrow, :], preferred_element_type=F32)
            gate_sums = g if t == 0 else gate_sums + g
            up_sums = u if t == 0 else up_sums + u
        return gate_sums / (1.0 + jnp.exp(-gate_sums)) * up_sums

    def compute(s):
        p = plane_at(s)
        if s == 0:
            for copy in loads[2:]:
                copy.wait()
            shared_hidden[...] = jnp.zeros_like(shared_hidden)
            shared_hidden[span(x * rows, rows), :] = hidden_of(lane * rows, rows, sg, su).astype(BF16)
        hidden = hidden_of(p * both, both, wg, wu)
        picks = lax.broadcasted_iota(jnp.int32, (wtb.shape[1], quarter), 0) == lane
        picks = picks.astype(F32).astype(BF16)
        weight = jnp.concatenate([
            lax.dot_general(wtb[p * 2 + i], picks, (((0,), (0,)), ((), ())), preferred_element_type=F32)
            for i in range(2)], axis=0)
        hidden = (hidden * weight).astype(BF16)
        for t in range(tensors):
            columns = slice(t * narrow, (t + 1) * narrow)
            value = jnp.dot(hidden, wd[:, columns], preferred_element_type=F32)
            if s == 0:
                value += jnp.dot(shared_hidden[...], sd[:, columns], preferred_element_type=F32)
            part[s, t] = value.astype(BF16)

    def add(count, dst, *sources):
        chunk = 32

        def step(i, carry):
            at = span(i * chunk, chunk)
            value = dst[at, :].astype(F32)
            for source in sources:
                value += source[at, :].astype(F32)
            dst[at, :] = value.astype(BF16)
            return carry

        lax.fori_loop(0, count // chunk, step, 0)

    def sum_piece(s, iy, ix):
        return part.at[s, iy * 2 + c, span(ix * rows, rows), :]

    def reduce_core(s):
        for i, iy in enumerate((oy, y)):
            send(("rc", i, s), part.at[s, iy * 2 + oc], got_core.at[s, iy], at_core)

    def reduce_far(s):
        for i in range(2):
            arrived(("rc", i, s))

        def side(iy, ix):
            add(rows, sum_piece(s, iy, ix), got_core.at[s, iy, span(ix * rows, rows), :])

        side(oy, ox)
        far = sum_piece(s, oy, ox)
        send(("r0", s), far.at[0:half, :], got_h0.at[s], at_y)
        send(("r1", s), far.at[half:rows, :], got_h1.at[s], at_x)
        side(y, ox)
        side(oy, x)
        side(y, x)

    def reduce_near(s):
        arrived(("r0", s))
        aside = sum_piece(s, y, ox)
        add(half, aside.at[0:half, :], got_h0.at[s])
        send(("rx", s), aside, got_x.at[s], at_x)
        arrived(("r1", s))
        across = sum_piece(s, oy, x)
        add(half, across.at[half:rows, :], got_h1.at[s])
        send(("ry", s), across, got_y.at[s], at_y)

    def reduce_ring(s, before):
        arrived(("rx", s))
        arrived(("ry", s))
        own = sum_piece(s, y, x)
        sources = [got_x.at[s], got_y.at[s]]
        if before is not None:
            arrived(("rz", before))
            sources.append(got_z.at[before])
        add(rows, own, *sources)
        if s == 0:
            out_ref[...] = own[...]
        else:
            send(("rz", s), own, got_z.at[s], at_up)

    last = planes - 1
    issue(0)
    forward(0)
    if last:
        issue(1)
    finish(0)
    compute(0)
    reduce_core(0)
    for s in range(1, planes):
        forward(s)
        if s < last:
            issue(s + 1)
        if s >= 2:
            reduce_far(s - 1)
        if s >= 3:
            reduce_near(s - 2)
        finish(s)
        compute(s)
        reduce_core(s)
    for s in range(max(1, last - 1), planes):
        if s == last:
            reduce_far(s)
            reduce_far(0)
        if s == last - 1:
            reduce_near(s)
    done = None
    for s in range(1, last):
        reduce_ring(s, done)
        done = s
    reduce_near(last)
    reduce_near(0)
    reduce_ring(last, done)
    reduce_ring(0, last)
    for copy in copies.values():
        copy.wait_send()


def kernel_form(
    tokens, expert_ids, gate_values, w_gate, w_up, w_down, shared_gate, shared_up, shared_down
):
    rows, narrow = tokens.shape
    unused, features, quarter = w_gate.shape
    lanes, tensors = lax.axis_size("expert"), lax.axis_size("tensor")
    planes = lanes // 2
    table = -(-lanes // 16) * 16
    numbers = jnp.arange(table, dtype=jnp.int32)[:, None, None]
    weights = jnp.sum(jnp.where(expert_ids[None] == numbers, gate_values[None].astype(F32), 0.0), axis=2)
    anywhere = pl.BlockSpec(memory_space=pl.ANY)
    shared_units = shared_gate.shape[1]
    count = 18 * planes
    return pl.pallas_call(
        functools.partial(layer_kernel, lanes),
        out_shape=jax.ShapeDtypeStruct((rows, narrow), BF16),
        in_specs=[anywhere] * 8,
        out_specs=pl.BlockSpec(memory_space=pltpu.VMEM),
        scratch_shapes=[
            pltpu.VMEM((tensors, lanes * rows, narrow), BF16),
            pltpu.VMEM((lanes, table, rows), BF16),
            pltpu.VMEM((features, quarter), BF16),
            pltpu.VMEM((features, quarter), BF16),
            pltpu.VMEM((quarter, features), BF16),
            pltpu.VMEM((features, shared_units), BF16),
            pltpu.VMEM((features, shared_units), BF16),
            pltpu.VMEM((shared_units, features), BF16),
            pltpu.VMEM((2 * rows, shared_units), BF16),
            pltpu.VMEM((planes, tensors, 2 * rows, narrow), BF16),
            pltpu.VMEM((planes, 2, 2 * rows, narrow), BF16),
            pltpu.VMEM((planes, rows // 2, narrow), BF16),
            pltpu.VMEM((planes, rows // 2, narrow), BF16),
            pltpu.VMEM((planes, rows, narrow), BF16),
            pltpu.VMEM((planes, rows, narrow), BF16),
            pltpu.VMEM((planes, rows, narrow), BF16),
            pltpu.SemaphoreType.DMA((8,)),
            pltpu.SemaphoreType.DMA((count,)),
            pltpu.SemaphoreType.DMA((count,)),
        ],
        compiler_params=pltpu.CompilerParams(
            collective_id=0, has_side_effects=True, vmem_limit_bytes=60 * 1024 * 1024
        ),
    )(tokens, weights.astype(BF16), w_gate[0], w_up[0], w_down[0], shared_gate, shared_up, shared_down)


def per_device(tokens, expert_ids, gate_values, w_gate, *rest):
    per_lane = w_gate.shape[0]
    lanes, tensors = lax.axis_size("expert"), lax.axis_size("tensor")
    top = expert_ids.shape[1]
    capacity = capacity_of(tokens.shape[0], top, lanes * per_lane)
    grouped = per_lane == 1 and tensors == 4 and lanes % 2 == 0 and lanes >= 8
    dense = grouped and 2 * capacity >= tokens.shape[0]
    form = kernel_form if dense else dispatch_form
    return form(tokens, expert_ids, gate_values, w_gate, *rest)


def solution(mesh):
    placed = (
        P("expert", "tensor"),
        P("expert", None),
        P("expert", None),
        P("expert", None, "tensor"),
        P("expert", None, "tensor"),
        P("expert", "tensor", None),
        P(None, "tensor"),
        P(None, "tensor"),
        P("tensor", None),
    )
    return jax.shard_map(
        per_device, mesh=mesh, in_specs=placed, out_specs=P("expert", "tensor"), check_vma=False
    )
```

```python
import functools

import jax
import jax.numpy as jnp
from jax import lax
from jax.experimental import pallas as pl
from jax.experimental.pallas import tpu as pltpu
from jax.sharding import PartitionSpec as P

MESH = pl.DeviceIdType.MESH
F32 = jnp.float32
BF16 = jnp.bfloat16


def capacity_of(tok_dev, top_count, experts_all):
    return min(tok_dev, 3 * tok_dev * top_count // (2 * experts_all))


def dispatch_form(
    tokens, expert_ids, gate_values, w_gate, w_up, w_down, shared_gate, shared_up, shared_down
):
    tok_dev, narrow = tokens.shape
    top_count = expert_ids.shape[1]
    per_lane, features, quarter = w_gate.shape
    lane_count = lax.axis_size("expert")
    experts_all = lane_count * per_lane
    capacity = min(tok_dev, 3 * tok_dev * top_count // (2 * experts_all))
    total_rows = experts_all * capacity
    numbers = jnp.arange(experts_all, dtype=jnp.int32)
    onehot = (expert_ids[:, :, None] == numbers).astype(jnp.int32)
    per_token = jnp.sum(onehot, axis=1)
    earlier = jnp.cumsum(per_token, axis=0) - per_token
    slot_index = jnp.sum(onehot * earlier[:, None, :], axis=2)
    target = expert_ids * capacity + slot_index
    token_index = jnp.repeat(jnp.arange(tok_dev, dtype=jnp.int32), top_count)
    owners = jnp.full((total_rows,), tok_dev, jnp.int32).at[target.reshape(-1)].set(token_index)
    features_all = lax.all_gather(tokens, "tensor", axis=1, tiled=True)
    shared_gate_sums = jnp.dot(features_all, shared_gate, preferred_element_type=jnp.float32)
    shared_up_sums = jnp.dot(features_all, shared_up, preferred_element_type=jnp.float32)
    shared_hidden = (jax.nn.silu(shared_gate_sums) * shared_up_sums).astype(jnp.bfloat16)
    shared_partial = jnp.dot(shared_hidden, shared_down, preferred_element_type=jnp.float32)
    padded = jnp.concatenate([tokens, jnp.zeros((1, narrow), jnp.bfloat16)], axis=0)
    outgoing = padded[owners].reshape(lane_count, per_lane * capacity, narrow)
    arrived = lax.all_to_all(outgoing, "expert", split_axis=0, concat_axis=0, tiled=True)
    arrived = arrived.reshape(lane_count, per_lane, capacity, narrow)
    block_rows = lax.all_gather(arrived, "tensor", axis=3, tiled=True)
    gate_more = jnp.einsum("sjcd,jdf->sjcf", block_rows, w_gate, preferred_element_type=jnp.float32)
    up_more = jnp.einsum("sjcd,jdf->sjcf", block_rows, w_up, preferred_element_type=jnp.float32)
    hidden = (jax.nn.silu(gate_more) * up_more).astype(jnp.bfloat16)
    partial_value = jnp.einsum("sjcf,jfd->sjcd", hidden, w_down, preferred_element_type=jnp.float32)
    summed = lax.psum_scatter(
        partial_value.astype(jnp.bfloat16), "tensor", scatter_dimension=3, tiled=True
    ).astype(jnp.float32)
    returned = lax.all_to_all(
        summed.reshape(lane_count, per_lane * capacity, narrow).astype(jnp.bfloat16),
        "expert",
        split_axis=0,
        concat_axis=0,
        tiled=True,
    ).astype(jnp.float32)
    picked = returned.reshape(total_rows, narrow)[target]
    routed = jnp.sum(gate_values.astype(jnp.float32)[:, :, None] * picked, axis=1)
    shared_total = lax.psum_scatter(
        shared_partial.astype(jnp.bfloat16), "tensor", scatter_dimension=1, tiled=True
    ).astype(jnp.float32)
    return (routed + shared_total).astype(jnp.bfloat16)


def layer_kernel(
    lanes, tok_hbm, wt_hbm, wg_hbm, wu_hbm, wd_hbm, sg_hbm, su_hbm, sd_hbm, out_ref,
    xbuf, wtb, wg, wu, wd, sg, su, sd, shared_hidden, part, got_core, got_h0, got_h1,
    got_x, got_y, got_z, got_far, load_sem, send_sem, recv_sem,
):
    planes = lanes // 2
    rows, narrow = out_ref.shape
    half, both = rows // 2, 2 * rows
    quarter = wg.shape[1]
    lane, tens = lax.axis_index("expert"), lax.axis_index("tensor")
    z, x = lane // 2, lax.rem(lane, 2)
    y, c = tens // 2, lax.rem(tens, 2)
    ox, oy, oc = 1 - x, 1 - y, 1 - c
    up = lax.rem(z + 1, planes)
    down = lax.rem(z + planes - 1, planes)
    at_core = (lane, y * 2 + oc)
    at_x = (z * 2 + ox, tens)
    at_y = (lane, oy * 2 + c)
    at_up = (up * 2 + x, tens)
    at_down = (down * 2 + x, tens)
    tens_y = oy * 2 + c
    number, copies = {}, {}
    gather_ring = range(planes - 2, planes)
    reduce_ring_far = range(0)

    def send(key, src, dst, device):
        k = number.setdefault(key, len(number))
        copies[key] = pltpu.make_async_remote_copy(
            src_ref=src, dst_ref=dst, send_sem=send_sem.at[k], recv_sem=recv_sem.at[k],
            device_id=device, device_id_type=MESH)
        copies[key].start()

    def arrived(key):
        copies[key].wait_recv()

    def span(start, size):
        return pl.ds(pl.multiple_of(start, size), size)

    def piece(t, plane, ix):
        return xbuf.at[t, span((plane * 2 + ix) * rows, rows), :]

    def half_piece(t, plane, ix, h):
        return xbuf.at[t, span((plane * 2 + ix) * rows + h * half, half), :]

    loads = []
    for src, dst in (
        (tok_hbm, piece(tens, z, x)), (wt_hbm, wtb.at[lane]), (wg_hbm, wg), (wu_hbm, wu),
        (sg_hbm, sg), (su_hbm, su), (wd_hbm, wd), (sd_hbm, sd),
    ):
        copy = pltpu.make_async_copy(src, dst, load_sem.at[len(loads)])
        copy.start()
        loads.append(copy)

    barrier = pltpu.get_barrier_semaphore()
    for device in (at_core, at_x, at_y, at_up, at_down):
        pl.semaphore_signal(barrier, inc=1, device_id=device, device_id_type=MESH)
    pl.semaphore_wait(barrier, 5)

    def plane_at(s):
        return lax.rem(z - s + planes, planes)

    def issue(s):
        p = plane_at(s)
        if s == 0:
            loads[0].wait()
            loads[1].wait()
        else:
            arrived(("z", s - 1))
            arrived(("wz", s - 1))
        mine, weight = piece(tens, p, x), wtb.at[p * 2 + x]
        if s < planes - 1:
            send(("z", s), mine, mine, at_up)
            send(("wz", s), weight, weight, at_up)
        for h in range(2):
            ahead, behind = half_piece(tens, p, x, h), half_piece(tens, p, x, 1 - h)
            send(("x", h, s), ahead, ahead, at_x)
            send(("y", 1 - h, s), behind, behind, at_y)
        send(("wx", s), weight, weight, at_x)
        send(("c", s), mine, mine, at_core)

    def forward(s):
        p = plane_at(s)
        arrived(("x", 0, s))
        if s not in gather_ring:
            first = half_piece(tens, p, ox, 0)
            send(("d0", s), first, first, at_y)
        arrived(("y", 1, s))
        if s not in gather_ring:
            second = half_piece(tens_y, p, x, 1)
            send(("d1", s), second, second, at_x)
        arrived(("x", 1, s))
        other = piece(tens, p, ox)
        send(("cx", s), other, other, at_core)
        arrived(("y", 0, s))
        other = piece(tens_y, p, x)
        send(("cy", s), other, other, at_core)

    def finish(s):
        p = plane_at(s)
        far = piece(tens_y, p, ox)
        if s in gather_ring:
            arrived(("zd", s - 1))
        else:
            arrived(("d0", s))
            arrived(("d1", s))
        if s + 1 in gather_ring:
            send(("zd", s), far, far, at_up)
        send(("cd", s), far, far, at_core)
        arrived(("wx", s))
        for key in ("c", "cx", "cy", "cd"):
            arrived((key, s))

    tensors = xbuf.shape[0]

    def hidden_of(start, count, gate_matrix, up_matrix):
        gate_sums = up_sums = None
        for t in range(tensors):
            block = xbuf[t, span(start, count), :]
            g = jnp.dot(block, gate_matrix[t * narrow:(t + 1) * narrow, :], preferred_element_type=F32)
            u = jnp.dot(block, up_matrix[t * narrow:(t + 1) * narrow, :], preferred_element_type=F32)
            gate_sums = g if t == 0 else gate_sums + g
            up_sums = u if t == 0 else up_sums + u
        return gate_sums / (1.0 + jnp.exp(-gate_sums)) * up_sums

    def compute(s):
        p = plane_at(s)
        if s == 0:
            for copy in loads[2:]:
                copy.wait()
            shared_hidden[...] = jnp.zeros_like(shared_hidden)
            shared_hidden[span(x * rows, rows), :] = hidden_of(lane * rows, rows, sg, su).astype(BF16)
        hidden = hidden_of(p * both, both, wg, wu)
        picks = lax.broadcasted_iota(jnp.int32, (wtb.shape[1], quarter), 0) == lane
        picks = picks.astype(F32).astype(BF16)
        weight = jnp.concatenate([
            lax.dot_general(wtb[p * 2 + i], picks, (((0,), (0,)), ((), ())), preferred_element_type=F32)
            for i in range(2)], axis=0)
        hidden = (hidden * weight).astype(BF16)
        for t in range(tensors):
            columns = slice(t * narrow, (t + 1) * narrow)
            value = jnp.dot(hidden, wd[:, columns], preferred_element_type=F32)
            if s == 0:
                value += jnp.dot(shared_hidden[...], sd[:, columns], preferred_element_type=F32)
            part[s, t] = value.astype(BF16)

    def add(count, dst, *sources):
        chunk = 32

        def step(i, carry):
            at = span(i * chunk, chunk)
            value = dst[at, :].astype(F32)
            for source in sources:
                value += source[at, :].astype(F32)
            dst[at, :] = value.astype(BF16)
            return carry

        lax.fori_loop(0, count // chunk, step, 0)

    def sum_piece(s, iy, ix):
        return part.at[s, iy * 2 + c, span(ix * rows, rows), :]

    def reduce_core(s):
        for i, iy in enumerate((oy, y)):
            send(("rc", i, s), part.at[s, iy * 2 + oc], got_core.at[s, iy], at_core)

    def reduce_far(s):
        for i in range(2):
            arrived(("rc", i, s))

        def side(iy, ix):
            add(rows, sum_piece(s, iy, ix), got_core.at[s, iy, span(ix * rows, rows), :])

        side(oy, ox)
        far = sum_piece(s, oy, ox)
        previous = planes - 1 if s == 0 else s - 1
        if previous in reduce_ring_far:
            arrived(("zf", previous))
            add(rows, far, got_far.at[previous])
        if s in reduce_ring_far:
            send(("zf", s), far, got_far.at[s], at_up)
        else:
            send(("r0", s), far.at[0:half, :], got_h0.at[s], at_y)
            send(("r1", s), far.at[half:rows, :], got_h1.at[s], at_x)
        side(y, ox)
        side(oy, x)
        side(y, x)

    def reduce_near(s):
        aside = sum_piece(s, y, ox)
        if s not in reduce_ring_far:
            arrived(("r0", s))
            add(half, aside.at[0:half, :], got_h0.at[s])
        send(("rx", s), aside, got_x.at[s], at_x)
        across = sum_piece(s, oy, x)
        if s not in reduce_ring_far:
            arrived(("r1", s))
            add(half, across.at[half:rows, :], got_h1.at[s])
        send(("ry", s), across, got_y.at[s], at_y)

    def reduce_ring(s, before):
        arrived(("rx", s))
        arrived(("ry", s))
        own = sum_piece(s, y, x)
        sources = [got_x.at[s], got_y.at[s]]
        if before is not None:
            arrived(("rz", before))
            sources.append(got_z.at[before])
        add(rows, own, *sources)
        if s == 0:
            out_ref[...] = own[...]
        else:
            send(("rz", s), own, got_z.at[s], at_up)

    last = planes - 1
    issue(0)
    forward(0)
    if last:
        issue(1)
    finish(0)
    compute(0)
    reduce_core(0)
    for s in range(1, planes):
        forward(s)
        if s < last:
            issue(s + 1)
        if s >= 2:
            reduce_far(s - 1)
        if s >= 3:
            reduce_near(s - 2)
        finish(s)
        compute(s)
        reduce_core(s)
    for s in range(max(1, last - 1), planes):
        if s == last:
            reduce_far(s)
            reduce_far(0)
        if s == last - 1:
            reduce_near(s)
    done = None
    for s in range(1, last):
        reduce_ring(s, done)
        done = s
    reduce_near(last)
    reduce_near(0)
    reduce_ring(last, done)
    reduce_ring(0, last)
    for copy in copies.values():
        copy.wait_send()


def kernel_form(
    tokens, expert_ids, gate_values, w_gate, w_up, w_down, shared_gate, shared_up, shared_down
):
    rows, narrow = tokens.shape
    unused, features, quarter = w_gate.shape
    lanes, tensors = lax.axis_size("expert"), lax.axis_size("tensor")
    planes = lanes // 2
    table = -(-lanes // 16) * 16
    numbers = jnp.arange(table, dtype=jnp.int32)[:, None, None]
    weights = jnp.sum(jnp.where(expert_ids[None] == numbers, gate_values[None].astype(F32), 0.0), axis=2)
    anywhere = pl.BlockSpec(memory_space=pl.ANY)
    shared_units = shared_gate.shape[1]
    count = 24 * planes
    return pl.pallas_call(
        functools.partial(layer_kernel, lanes),
        out_shape=jax.ShapeDtypeStruct((rows, narrow), BF16),
        in_specs=[anywhere] * 8,
        out_specs=pl.BlockSpec(memory_space=pltpu.VMEM),
        scratch_shapes=[
            pltpu.VMEM((tensors, lanes * rows, narrow), BF16),
            pltpu.VMEM((lanes, table, rows), BF16),
            pltpu.VMEM((features, quarter), BF16),
            pltpu.VMEM((features, quarter), BF16),
            pltpu.VMEM((quarter, features), BF16),
            pltpu.VMEM((features, shared_units), BF16),
            pltpu.VMEM((features, shared_units), BF16),
            pltpu.VMEM((shared_units, features), BF16),
            pltpu.VMEM((2 * rows, shared_units), BF16),
            pltpu.VMEM((planes, tensors, 2 * rows, narrow), BF16),
            pltpu.VMEM((planes, 2, 2 * rows, narrow), BF16),
            pltpu.VMEM((planes, rows // 2, narrow), BF16),
            pltpu.VMEM((planes, rows // 2, narrow), BF16),
            pltpu.VMEM((planes, rows, narrow), BF16),
            pltpu.VMEM((planes, rows, narrow), BF16),
            pltpu.VMEM((planes, rows, narrow), BF16),
            pltpu.VMEM((planes, rows, narrow), BF16),
            pltpu.SemaphoreType.DMA((8,)),
            pltpu.SemaphoreType.DMA((count,)),
            pltpu.SemaphoreType.DMA((count,)),
        ],
        compiler_params=pltpu.CompilerParams(
            collective_id=0, has_side_effects=True, vmem_limit_bytes=60 * 1024 * 1024
        ),
    )(tokens, weights.astype(BF16), w_gate[0], w_up[0], w_down[0], shared_gate, shared_up, shared_down)


def per_device(tokens, expert_ids, gate_values, w_gate, *rest):
    per_lane = w_gate.shape[0]
    lanes, tensors = lax.axis_size("expert"), lax.axis_size("tensor")
    top = expert_ids.shape[1]
    capacity = capacity_of(tokens.shape[0], top, lanes * per_lane)
    grouped = per_lane == 1 and tensors == 4 and lanes % 2 == 0 and lanes >= 8
    dense = grouped and 2 * capacity >= tokens.shape[0]
    form = kernel_form if dense else dispatch_form
    return form(tokens, expert_ids, gate_values, w_gate, *rest)


def solution(mesh):
    placed = (
        P("expert", "tensor"),
        P("expert", None),
        P("expert", None),
        P("expert", None, "tensor"),
        P("expert", None, "tensor"),
        P("expert", "tensor", None),
        P(None, "tensor"),
        P(None, "tensor"),
        P("tensor", None),
    )
    return jax.shard_map(
        per_device, mesh=mesh, in_specs=placed, out_specs=P("expert", "tensor"), check_vma=False
    )
```

```python
import functools

import jax
import jax.numpy as jnp
from jax import lax
from jax.experimental import pallas as pl
from jax.experimental.pallas import tpu as pltpu
from jax.sharding import PartitionSpec as P

MESH = pl.DeviceIdType.MESH
F32 = jnp.float32
BF16 = jnp.bfloat16


def capacity_of(tok_dev, top_count, experts_all):
    return min(tok_dev, 3 * tok_dev * top_count // (2 * experts_all))


def dispatch_form(
    tokens, expert_ids, gate_values, w_gate, w_up, w_down, shared_gate, shared_up, shared_down
):
    tok_dev, narrow = tokens.shape
    top_count = expert_ids.shape[1]
    per_lane, features, quarter = w_gate.shape
    lane_count = lax.axis_size("expert")
    experts_all = lane_count * per_lane
    capacity = min(tok_dev, 3 * tok_dev * top_count // (2 * experts_all))
    total_rows = experts_all * capacity
    numbers = jnp.arange(experts_all, dtype=jnp.int32)
    onehot = (expert_ids[:, :, None] == numbers).astype(jnp.int32)
    per_token = jnp.sum(onehot, axis=1)
    earlier = jnp.cumsum(per_token, axis=0) - per_token
    slot_index = jnp.sum(onehot * earlier[:, None, :], axis=2)
    target = expert_ids * capacity + slot_index
    token_index = jnp.repeat(jnp.arange(tok_dev, dtype=jnp.int32), top_count)
    owners = jnp.full((total_rows,), tok_dev, jnp.int32).at[target.reshape(-1)].set(token_index)
    features_all = lax.all_gather(tokens, "tensor", axis=1, tiled=True)
    shared_gate_sums = jnp.dot(features_all, shared_gate, preferred_element_type=jnp.float32)
    shared_up_sums = jnp.dot(features_all, shared_up, preferred_element_type=jnp.float32)
    shared_hidden = (jax.nn.silu(shared_gate_sums) * shared_up_sums).astype(jnp.bfloat16)
    shared_partial = jnp.dot(shared_hidden, shared_down, preferred_element_type=jnp.float32)
    padded = jnp.concatenate([tokens, jnp.zeros((1, narrow), jnp.bfloat16)], axis=0)
    outgoing = padded[owners].reshape(lane_count, per_lane * capacity, narrow)
    arrived = lax.all_to_all(outgoing, "expert", split_axis=0, concat_axis=0, tiled=True)
    arrived = arrived.reshape(lane_count, per_lane, capacity, narrow)
    block_rows = lax.all_gather(arrived, "tensor", axis=3, tiled=True)
    gate_more = jnp.einsum("sjcd,jdf->sjcf", block_rows, w_gate, preferred_element_type=jnp.float32)
    up_more = jnp.einsum("sjcd,jdf->sjcf", block_rows, w_up, preferred_element_type=jnp.float32)
    hidden = (jax.nn.silu(gate_more) * up_more).astype(jnp.bfloat16)
    partial_value = jnp.einsum("sjcf,jfd->sjcd", hidden, w_down, preferred_element_type=jnp.float32)
    summed = lax.psum_scatter(
        partial_value.astype(jnp.bfloat16), "tensor", scatter_dimension=3, tiled=True
    ).astype(jnp.float32)
    returned = lax.all_to_all(
        summed.reshape(lane_count, per_lane * capacity, narrow).astype(jnp.bfloat16),
        "expert",
        split_axis=0,
        concat_axis=0,
        tiled=True,
    ).astype(jnp.float32)
    picked = returned.reshape(total_rows, narrow)[target]
    routed = jnp.sum(gate_values.astype(jnp.float32)[:, :, None] * picked, axis=1)
    shared_total = lax.psum_scatter(
        shared_partial.astype(jnp.bfloat16), "tensor", scatter_dimension=1, tiled=True
    ).astype(jnp.float32)
    return (routed + shared_total).astype(jnp.bfloat16)


def layer_kernel(
    lanes, tok_hbm, wt_hbm, wg_hbm, wu_hbm, wd_hbm, sg_hbm, su_hbm, sd_hbm, out_ref,
    xbuf, wtb, wg, wu, wd, sg, su, sd, shared_hidden, part, got_core, got_h0, got_h1,
    got_x, got_y, got_z, got_far, load_sem, send_sem, recv_sem,
):
    planes = lanes // 2
    rows, narrow = out_ref.shape
    half, both = rows // 2, 2 * rows
    quarter = wg.shape[1]
    lane, tens = lax.axis_index("expert"), lax.axis_index("tensor")
    z, x = lane // 2, lax.rem(lane, 2)
    y, c = tens // 2, lax.rem(tens, 2)
    ox, oy, oc = 1 - x, 1 - y, 1 - c
    up = lax.rem(z + 1, planes)
    down = lax.rem(z + planes - 1, planes)
    at_core = (lane, y * 2 + oc)
    at_x = (z * 2 + ox, tens)
    at_y = (lane, oy * 2 + c)
    at_up = (up * 2 + x, tens)
    at_down = (down * 2 + x, tens)
    tens_y = oy * 2 + c
    number, copies = {}, {}
    gather_ring = range(planes - 2, planes)
    reduce_ring_far = range(0)

    def send(key, src, dst, device):
        k = number.setdefault(key, len(number))
        copies[key] = pltpu.make_async_remote_copy(
            src_ref=src, dst_ref=dst, send_sem=send_sem.at[k], recv_sem=recv_sem.at[k],
            device_id=device, device_id_type=MESH)
        copies[key].start()

    def arrived(key):
        copies[key].wait_recv()

    def span(start, size):
        return pl.ds(pl.multiple_of(start, size), size)

    def piece(t, plane, ix):
        return xbuf.at[t, span((plane * 2 + ix) * rows, rows), :]

    def half_piece(t, plane, ix, h):
        return xbuf.at[t, span((plane * 2 + ix) * rows + h * half, half), :]

    loads = []
    for src, dst in (
        (tok_hbm, piece(tens, z, x)), (wt_hbm, wtb.at[lane]), (wg_hbm, wg), (wu_hbm, wu),
        (sg_hbm, sg), (su_hbm, su), (wd_hbm, wd), (sd_hbm, sd),
    ):
        copy = pltpu.make_async_copy(src, dst, load_sem.at[len(loads)])
        copy.start()
        loads.append(copy)

    barrier = pltpu.get_barrier_semaphore()
    for device in (at_core, at_x, at_y, at_up, at_down):
        pl.semaphore_signal(barrier, inc=1, device_id=device, device_id_type=MESH)
    pl.semaphore_wait(barrier, 5)

    def plane_at(s):
        return lax.rem(z - s + planes, planes)

    def issue(s):
        p = plane_at(s)
        if s == 0:
            loads[0].wait()
            loads[1].wait()
        else:
            arrived(("z", s - 1))
            arrived(("wz", s - 1))
        mine, weight = piece(tens, p, x), wtb.at[p * 2 + x]
        if s < planes - 1:
            send(("z", s), mine, mine, at_up)
            send(("wz", s), weight, weight, at_up)
        for h in range(2):
            ahead, behind = half_piece(tens, p, x, h), half_piece(tens, p, x, 1 - h)
            send(("x", h, s), ahead, ahead, at_x)
            send(("y", 1 - h, s), behind, behind, at_y)
        send(("wx", s), weight, weight, at_x)
        send(("c", s), mine, mine, at_core)

    def forward(s):
        p = plane_at(s)
        arrived(("x", 0, s))
        if s not in gather_ring:
            first = half_piece(tens, p, ox, 0)
            send(("d0", s), first, first, at_y)
        arrived(("y", 1, s))
        if s not in gather_ring:
            second = half_piece(tens_y, p, x, 1)
            send(("d1", s), second, second, at_x)
        arrived(("x", 1, s))
        other = piece(tens, p, ox)
        send(("cx", s), other, other, at_core)
        arrived(("y", 0, s))
        other = piece(tens_y, p, x)
        send(("cy", s), other, other, at_core)

    def finish(s):
        p = plane_at(s)
        far = piece(tens_y, p, ox)
        if s in gather_ring:
            arrived(("zd", s - 1))
        else:
            arrived(("d0", s))
            arrived(("d1", s))
        if s + 1 in gather_ring:
            send(("zd", s), far, far, at_up)
        send(("cd", s), far, far, at_core)
        arrived(("wx", s))
        for key in ("c", "cx", "cy", "cd"):
            arrived((key, s))

    tensors = xbuf.shape[0]

    def hidden_of(start, count, gate_matrix, up_matrix):
        gate_sums = up_sums = None
        for t in range(tensors):
            block = xbuf[t, span(start, count), :]
            g = jnp.dot(block, gate_matrix[t * narrow:(t + 1) * narrow, :], preferred_element_type=F32)
            u = jnp.dot(block, up_matrix[t * narrow:(t + 1) * narrow, :], preferred_element_type=F32)
            gate_sums = g if t == 0 else gate_sums + g
            up_sums = u if t == 0 else up_sums + u
        return gate_sums / (1.0 + jnp.exp(-gate_sums)) * up_sums

    def compute(s):
        p = plane_at(s)
        if s == 0:
            for copy in loads[2:]:
                copy.wait()
            shared_hidden[...] = jnp.zeros_like(shared_hidden)
            shared_hidden[span(x * rows, rows), :] = hidden_of(lane * rows, rows, sg, su).astype(BF16)
        hidden = hidden_of(p * both, both, wg, wu)
        picks = lax.broadcasted_iota(jnp.int32, (wtb.shape[1], quarter), 0) == lane
        picks = picks.astype(F32).astype(BF16)
        weight = jnp.concatenate([
            lax.dot_general(wtb[p * 2 + i], picks, (((0,), (0,)), ((), ())), preferred_element_type=F32)
            for i in range(2)], axis=0)
        hidden = (hidden * weight).astype(BF16)
        for t in range(tensors):
            columns = slice(t * narrow, (t + 1) * narrow)
            value = jnp.dot(hidden, wd[:, columns], preferred_element_type=F32)
            if s == 0:
                value += jnp.dot(shared_hidden[...], sd[:, columns], preferred_element_type=F32)
            part[s, t] = value.astype(BF16)

    def add(count, dst, *sources):
        chunk = 32

        def step(i, carry):
            at = span(i * chunk, chunk)
            value = dst[at, :].astype(F32)
            for source in sources:
                value += source[at, :].astype(F32)
            dst[at, :] = value.astype(BF16)
            return carry

        lax.fori_loop(0, count // chunk, step, 0)

    def sum_piece(s, iy, ix):
        return part.at[s, iy * 2 + c, span(ix * rows, rows), :]

    def reduce_core(s):
        for i, iy in enumerate((oy, y)):
            send(("rc", i, s), part.at[s, iy * 2 + oc], got_core.at[s, iy], at_core)

    def reduce_far(s):
        for i in range(2):
            arrived(("rc", i, s))

        def side(iy, ix):
            add(rows, sum_piece(s, iy, ix), got_core.at[s, iy, span(ix * rows, rows), :])

        side(oy, ox)
        far = sum_piece(s, oy, ox)
        previous = planes - 1 if s == 0 else s - 1
        if previous in reduce_ring_far:
            arrived(("zf", previous))
            add(rows, far, got_far.at[previous])
        if s in reduce_ring_far:
            send(("zf", s), far, got_far.at[s], at_up)
        else:
            send(("r0", s), far.at[0:half, :], got_h0.at[s], at_y)
            send(("r1", s), far.at[half:rows, :], got_h1.at[s], at_x)
        side(y, ox)
        side(oy, x)
        side(y, x)

    def reduce_near(s):
        aside = sum_piece(s, y, ox)
        if s not in reduce_ring_far:
            arrived(("r0", s))
            add(half, aside.at[0:half, :], got_h0.at[s])
        send(("rx", s), aside, got_x.at[s], at_x)
        across = sum_piece(s, oy, x)
        if s not in reduce_ring_far:
            arrived(("r1", s))
            add(half, across.at[half:rows, :], got_h1.at[s])
        send(("ry", s), across, got_y.at[s], at_y)

    def reduce_ring(s, before):
        arrived(("rx", s))
        arrived(("ry", s))
        own = sum_piece(s, y, x)
        sources = [got_x.at[s], got_y.at[s]]
        if before is not None:
            arrived(("rz", before))
            sources.append(got_z.at[before])
        add(rows, own, *sources)
        if s == 0:
            out_ref[...] = own[...]
        else:
            send(("rz", s), own, got_z.at[s], at_up)

    last = planes - 1
    issue(0)
    forward(0)
    if last:
        issue(1)
    finish(0)
    forward(1)
    issue(2)
    compute(0)
    reduce_core(0)
    for s in range(1, planes):
        if s >= 2:
            forward(s)
            if s < last:
                issue(s + 1)
            reduce_far(s - 1)
        if s >= 3:
            reduce_near(s - 2)
        finish(s)
        compute(s)
        reduce_core(s)
    for s in range(max(1, last - 1), planes):
        if s == last:
            reduce_far(s)
            reduce_far(0)
        if s == last - 1:
            reduce_near(s)
    done = None
    for s in range(1, last):
        reduce_ring(s, done)
        done = s
    reduce_near(last)
    reduce_near(0)
    reduce_ring(last, done)
    reduce_ring(0, last)
    for copy in copies.values():
        copy.wait_send()


def kernel_form(
    tokens, expert_ids, gate_values, w_gate, w_up, w_down, shared_gate, shared_up, shared_down
):
    rows, narrow = tokens.shape
    unused, features, quarter = w_gate.shape
    lanes, tensors = lax.axis_size("expert"), lax.axis_size("tensor")
    planes = lanes // 2
    table = -(-lanes // 16) * 16
    numbers = jnp.arange(table, dtype=jnp.int32)[:, None, None]
    weights = jnp.sum(jnp.where(expert_ids[None] == numbers, gate_values[None].astype(F32), 0.0), axis=2)
    anywhere = pl.BlockSpec(memory_space=pl.ANY)
    shared_units = shared_gate.shape[1]
    count = 24 * planes
    return pl.pallas_call(
        functools.partial(layer_kernel, lanes),
        out_shape=jax.ShapeDtypeStruct((rows, narrow), BF16),
        in_specs=[anywhere] * 8,
        out_specs=pl.BlockSpec(memory_space=pltpu.VMEM),
        scratch_shapes=[
            pltpu.VMEM((tensors, lanes * rows, narrow), BF16),
            pltpu.VMEM((lanes, table, rows), BF16),
            pltpu.VMEM((features, quarter), BF16),
            pltpu.VMEM((features, quarter), BF16),
            pltpu.VMEM((quarter, features), BF16),
            pltpu.VMEM((features, shared_units), BF16),
            pltpu.VMEM((features, shared_units), BF16),
            pltpu.VMEM((shared_units, features), BF16),
            pltpu.VMEM((2 * rows, shared_units), BF16),
            pltpu.VMEM((planes, tensors, 2 * rows, narrow), BF16),
            pltpu.VMEM((planes, 2, 2 * rows, narrow), BF16),
            pltpu.VMEM((planes, rows // 2, narrow), BF16),
            pltpu.VMEM((planes, rows // 2, narrow), BF16),
            pltpu.VMEM((planes, rows, narrow), BF16),
            pltpu.VMEM((planes, rows, narrow), BF16),
            pltpu.VMEM((planes, rows, narrow), BF16),
            pltpu.VMEM((planes, rows, narrow), BF16),
            pltpu.SemaphoreType.DMA((8,)),
            pltpu.SemaphoreType.DMA((count,)),
            pltpu.SemaphoreType.DMA((count,)),
        ],
        compiler_params=pltpu.CompilerParams(
            collective_id=0, has_side_effects=True, vmem_limit_bytes=60 * 1024 * 1024
        ),
    )(tokens, weights.astype(BF16), w_gate[0], w_up[0], w_down[0], shared_gate, shared_up, shared_down)


def per_device(tokens, expert_ids, gate_values, w_gate, *rest):
    per_lane = w_gate.shape[0]
    lanes, tensors = lax.axis_size("expert"), lax.axis_size("tensor")
    top = expert_ids.shape[1]
    capacity = capacity_of(tokens.shape[0], top, lanes * per_lane)
    grouped = per_lane == 1 and tensors == 4 and lanes % 2 == 0 and lanes >= 8
    dense = grouped and 2 * capacity >= tokens.shape[0]
    form = kernel_form if dense else dispatch_form
    return form(tokens, expert_ids, gate_values, w_gate, *rest)


def solution(mesh):
    placed = (
        P("expert", "tensor"),
        P("expert", None),
        P("expert", None),
        P("expert", None, "tensor"),
        P("expert", None, "tensor"),
        P("expert", "tensor", None),
        P(None, "tensor"),
        P(None, "tensor"),
        P("tensor", None),
    )
    return jax.shard_map(
        per_device, mesh=mesh, in_specs=placed, out_specs=P("expert", "tensor"), check_vma=False
    )
```
